32 devices in a mesh: groups: 2 (over y), seq: 4 (over z), head: 4 (over x, core).
Axes of the slice: x: 2, y: 2, z: 4, core: 2. Of those that a mesh axis runs over, the one named last changes fastest.
Arguments:
- tile_tokens: bfloat16 [16, 256, 1536], P(('groups', 'seq')), parts along dimension 0, may hold values from -6 to 6
- tile_gain: float32 [1536], replicated, may hold values from 0.1 to 1.9
- w_gate_up: bfloat16 [2, 1536, 4096], P(None, 'seq', 'head'), may hold values from -0.15625 to 0.15625
- w_down: bfloat16 [4096, 1536], P('head', 'seq'), may hold values from -0.09375 to 0.09375
- layer_scale: float32 [1536], replicated, may hold values from 1 to 8
- fc_gain: float32 [1536], replicated, may hold values from 0.1 to 1.9
- w_embed: bfloat16 [1536, 768], P(None, 'head'), may hold values from -0.15625 to 0.15625
- embed_bias: float32 [768], P('head'), may hold values from -3 to 3
- pre_emb: bfloat16 [2032, 768], P(('groups', 'seq'), 'head'), parts along dimension 0, may hold values from -6 to 6
- tile_order: int32 [2048], P('groups'), parts along dimension 0, may hold values from 0 to 1023, as said below
- valid_count: int32 [2], P('groups'), parts along dimension 0, may hold values from 256 to 1024
- slide_gain: float32 [768], replicated, may hold values from 0.1 to 1.9
- w_qkv: bfloat16 [3, 768, 768], P(None, None, 'head'), may hold values from -1.25 to 1.25
- sub_gain: float32 [768], P('head'), may hold values from 0.1 to 1.9
- w_out: bfloat16 [768, 768], P('head'), may hold values from -0.21875 to 0.21875
Outputs:
- mixed: float32 [2048, 768], P(('groups', 'seq'), 'head'), parts along dimension 0
The draws below stay inside these ranges and needn't reach their ends.
There are 2 independent parts, one for each index of `groups`. The reference program is written for one: setup_inputs(seed, part) draws one part's arguments, and reference() takes and returns one part's arrays. A program takes and returns all parts, laid end to end along the dimension named above; an argument that names none is the same for every part. Nothing has to cross between parts.
Inputs may be any that keep to these rules, and one draw needn't show every extreme that they name: `tile_order`: A permutation of 0 to 1023. For every block of 256 positions (d * 256 to (d + 1) * 256 - 1) and every block of 256 stored rows, exactly 64 positions of the first take rows of the second.
All inputs are finite; a program needn't handle non-finite values.
Results may differ from the reference program's by a relative error of at most 0.0046.
Values may be sent and summed in bfloat16 or wider, within the bound.
No kernel may reach another device: no remote copies, remote signals or barrier semaphores. Data moves between devices by JAX's collectives and lax.ppermute only.
A program may use at most 64 MiB of HBM per device.

```python
import math
import jax
import jax.numpy as jnp
from jax import lax

DV = 1536
FF = 4096
DS = 768
HEADS = 16
HEAD_DIM = 48
PATCH = 256
NEW_DEV = 2
SEQ_DEV = 256
DILATION_SECOND = 4
DILATION_THIRD = 16
NEW = 8
PRE_DEV = 254
PRE = 1016
SLIDE_POSITIONS = 1024
PEER = 64
SEGMENT_FIRST = 1024
SEGMENT_SECOND = 1024


def shuffle_row(row_key, row_values):
    return jax.random.permutation(row_key, row_values)


def draw_tile_order(key, part):
    blocks = SLIDE_POSITIONS // SEQ_DEV
    source_key, target_key = jax.random.split(jax.random.fold_in(key, 11))
    source_keys = jax.random.split(source_key, blocks)
    local_rows = jnp.broadcast_to(jnp.arange(SEQ_DEV, dtype=jnp.int32), (blocks, SEQ_DEV))
    shuffled = jax.vmap(shuffle_row)(source_keys, local_rows)
    stored = shuffled + (jnp.arange(blocks, dtype=jnp.int32) * SEQ_DEV)[:, None]
    arriving = stored.reshape(blocks, blocks, PEER).transpose(1, 0, 2).reshape(blocks, SEQ_DEV)
    target_keys = jax.random.split(target_key, blocks)
    placed = jax.vmap(shuffle_row)(target_keys, arriving)
    return placed.reshape(SLIDE_POSITIONS).astype(jnp.int32)


def draw_w_qkv(key, part):
    query_key = jax.random.fold_in(jax.random.fold_in(key, 7), 0)
    stacked = jax.random.normal(query_key, (3, DS, DS), jnp.float32) / math.sqrt(DS)
    return jnp.clip(stacked, -1.25, 1.25).astype(jnp.bfloat16)


def shard_levels(own_key, dims, pieces, low, high):
    level, own = 1.0, jax.random.fold_in(own_key, 6)
    for position, blocks in pieces:
        steps = jnp.exp(jax.random.uniform(jax.random.fold_in(own, position), (blocks,), jnp.float32, low / len(pieces), high / len(pieces)))
        level = level * jnp.repeat(steps, dims[position] // blocks).reshape([-1 if axis == position else 1 for axis in range(len(dims))])
    return level


def centred(own_key, extent, deviation, reach, cuts=(), kind=jnp.bfloat16):
    values = jax.random.normal(own_key, extent, jnp.float32) * deviation
    if len(cuts) > 0:
        values = shard_levels(own_key, extent, cuts, -0.22, 0.18) * values
    return jnp.clip(values, min=-reach, max=reach).astype(kind)


def setup_inputs(seed: int = 0, part: int = 0) -> dict:
    key_of = jax.random.split(jax.random.key(seed), 16)
    part_splits = jax.random.split(jax.random.fold_in(key_of[15], part), 16)
    return {
        "tile_tokens": centred(part_splits[0], (NEW, PATCH, DV), 1.0, 6.0, ((0, 4),)),
        "tile_gain": jnp.clip(1.0 + 0.18 * jax.random.normal(key_of[1], (DV,), jnp.float32), 0.1, 1.9),
        "w_gate_up": centred(key_of[2], (2, DV, FF), DV ** -0.5, 0.15625, ((1, 4), (2, 4))),
        "w_down": centred(key_of[3], (FF, DV), FF ** -0.5, 0.09375, ((0, 4), (1, 4))),
        "layer_scale": jnp.clip(jnp.exp(jax.random.uniform(key_of[4], (DV,), jnp.float32, math.log(1.0), math.log(8.0))), 1.0, 8.0),
        "fc_gain": jnp.clip(1.0 + 0.18 * jax.random.normal(key_of[5], (DV,), jnp.float32), 0.1, 1.9),
        "w_embed": centred(key_of[6], (DV, DS), DV ** -0.5, 0.15625, ((1, 4),)),
        "embed_bias": centred(key_of[7], (DS,), 0.5, 3.0, ((0, 4),), jnp.float32),
        "pre_emb": centred(part_splits[8], (PRE, DS), 1.0, 6.0, ((0, 4), (1, 4))),
        "tile_order": draw_tile_order(jax.random.fold_in(jax.random.fold_in(key_of[15], part), 71), part),
        "valid_count": jax.random.randint(part_splits[10], (1,), SLIDE_POSITIONS // 4, SLIDE_POSITIONS + 1).astype(jnp.int32),
        "slide_gain": jnp.clip(1.0 + 0.18 * jax.random.normal(key_of[11], (DS,), jnp.float32), 0.1, 1.9),
        "w_qkv": draw_w_qkv(jax.random.fold_in(key_of[15], 71), part),
        "sub_gain": jnp.clip(1.0 + 0.18 * jax.random.normal(key_of[13], (DS,), jnp.float32), 0.1, 1.9),
        "w_out": centred(key_of[14], (DS, DS), DS ** -0.5, 0.21875, ((0, 4),)),
    }


layer_eps = 1e-05
masked_score = -1e+30

def normalize(values, gain):
    centered = values - lax.optimization_barrier(jnp.mean(values, axis=-1, keepdims=True))
    variance = lax.optimization_barrier(jnp.mean(centered * centered, axis=-1, keepdims=True))
    return centered * lax.rsqrt(variance + layer_eps) * gain

def dilated_level(projected_rows, valid_limit, segment, dilation):
    seg_count = SLIDE_POSITIONS // segment
    seg_width = segment // dilation
    offsets = jnp.arange(HEADS, dtype=jnp.int32) % dilation
    choose = jnp.arange(dilation, dtype=jnp.int32)[:, None] == offsets[None, :]
    arranged = projected_rows.reshape(3, seg_count, seg_width, dilation, HEADS, HEAD_DIM)
    sparse = lax.optimization_barrier(jnp.sum(jnp.where(choose[None, None, None, :, :, None], arranged, jnp.zeros((), projected_rows.dtype)), axis=3))
    starts = jnp.arange(seg_count, dtype=jnp.int32) * segment
    steps_in = jnp.arange(seg_width, dtype=jnp.int32) * dilation
    key_pos = starts[:, None, None] + steps_in[None, :, None] + offsets[None, None, :]

    def one_segment(inputs):
        query_rows, key_rows, value_rows, positions = inputs
        scores = jnp.einsum('qhe,khe->hqk', query_rows.astype(jnp.float32), key_rows.astype(jnp.float32)) / math.sqrt(HEAD_DIM)
        scores = jnp.where((positions < valid_limit).T[:, None, :], scores, masked_score)
        highest = lax.optimization_barrier(jnp.max(scores, axis=-1, keepdims=True))
        exponent = jnp.exp(scores - highest)
        mass_sum = lax.optimization_barrier(jnp.sum(exponent, axis=-1, keepdims=True))
        weights = (exponent / mass_sum).astype(jnp.bfloat16)
        attended = jnp.einsum('hqk,khe->qhe', weights.astype(jnp.float32), value_rows.astype(jnp.float32))
        return (attended, (highest[..., 0] + jnp.log(mass_sum[..., 0])).T)
    attended, log_mass = lax.map(one_segment, (sparse[0], sparse[1], sparse[2], key_pos))
    spread_out = jnp.where(choose[None, None, :, :, None], attended[:, :, None, :, :], 0.0).reshape(SLIDE_POSITIONS, HEADS, HEAD_DIM)
    spread_mass = jnp.where(choose[None, None, :, :], log_mass[:, :, None, :], masked_score).reshape(SLIDE_POSITIONS, HEADS)
    selected = jnp.broadcast_to(choose[None, None, :, :], (seg_count, seg_width, dilation, HEADS)).reshape(SLIDE_POSITIONS, HEADS)
    return (spread_out, spread_mass, selected)

def reference(tile_tokens, tile_gain, w_gate_up, w_down, layer_scale, fc_gain, w_embed, embed_bias, pre_emb, tile_order, valid_count, slide_gain, w_qkv, sub_gain, w_out):

    def tile_layer(tile_rows):
        normed = normalize(tile_rows.astype(jnp.float32), tile_gain).astype(jnp.bfloat16)
        gate_part = jnp.dot(normed, w_gate_up[0], preferred_element_type=jnp.float32)
        upward = jnp.dot(normed, w_gate_up[1], preferred_element_type=jnp.float32)
        hidden = (jax.nn.silu(gate_part) * upward).astype(jnp.bfloat16)
        mlp_out = jnp.dot(hidden, w_down, preferred_element_type=jnp.float32)
        return lax.optimization_barrier(jnp.mean(tile_rows.astype(jnp.float32) + layer_scale * mlp_out, axis=0))
    pooled = lax.map(tile_layer, tile_tokens)
    feature = normalize(pooled, fc_gain).astype(jnp.bfloat16)
    new_rows = (jnp.dot(feature, w_embed, preferred_element_type=jnp.float32) + embed_bias).astype(jnp.bfloat16)
    blocks = SLIDE_POSITIONS // SEQ_DEV
    stored = jnp.concatenate([new_rows.reshape(blocks, NEW_DEV, DS), pre_emb.reshape(blocks, PRE_DEV, DS)], axis=1).reshape(SLIDE_POSITIONS, DS)
    sequence = jnp.take(stored, tile_order, axis=0)
    slide_normed = normalize(sequence.astype(jnp.float32), slide_gain).astype(jnp.bfloat16)
    projected_rows = jnp.stack([jnp.dot(slide_normed, w_qkv[which_one], preferred_element_type=jnp.float32).astype(jnp.bfloat16) for which_one in range(3)])
    valid_limit = valid_count[0]
    level_list = ((SEGMENT_FIRST, 1), (SEGMENT_SECOND, DILATION_SECOND), (SLIDE_POSITIONS, DILATION_THIRD))
    results = [dilated_level(projected_rows, valid_limit, segment, dilation) for segment, dilation in level_list]
    outputs = jnp.stack([level_result[0] for level_result in results])
    masses = jnp.stack([level_result[1] for level_result in results])
    selects = jnp.stack([level_result[2] for level_result in results])
    ceiling = lax.optimization_barrier(jnp.max(masses, axis=0))
    shares = jnp.where(selects, jnp.exp(masses - ceiling), 0.0)
    combined = lax.optimization_barrier(jnp.sum(shares[..., None] * outputs, axis=0)) / lax.optimization_barrier(jnp.sum(shares, axis=0))[..., None]
    positions = jnp.arange(SLIDE_POSITIONS, dtype=jnp.int32)
    combined = jnp.where((positions < valid_limit)[:, None, None], combined, 0.0).reshape(SLIDE_POSITIONS, DS)
    mean_value = lax.optimization_barrier(jnp.mean(combined, axis=1, keepdims=True))
    mean_square = lax.optimization_barrier(jnp.mean(combined * combined, axis=1, keepdims=True))
    settled = ((combined - mean_value) * lax.rsqrt(mean_square - mean_value * mean_value + layer_eps) * sub_gain).astype(jnp.bfloat16)
    return sequence.astype(jnp.float32) + jnp.dot(settled, w_out, preferred_element_type=jnp.float32)
```

```python
import math

import jax
import jax.numpy as jnp
from jax import lax
from jax.sharding import PartitionSpec as P

DS = 768
HEAD_DIM = 48
SPAN0 = 1024
SPAN1 = 4096
DILATION_SECOND = 4
DILATION_THIRD = 16


layer_eps = 1e-05
masked_score = -1e30


def from_partner(value, axis, bit):
    mask = 2**bit
    pairs = [(source, source ^ mask) for source in range(lax.axis_size(axis))]
    return lax.ppermute(value, axis, pairs)


def normalize(values, gain):
    centered = values - jnp.mean(values, axis=-1, keepdims=True)
    variance = jnp.mean(centered * centered, axis=-1, keepdims=True)
    return centered * lax.rsqrt(variance + layer_eps) * gain


def select_rows(stacked, dilation, offsets):
    group_count, row_count, row_width = stacked.shape
    head_count = offsets.shape[0]
    arranged = stacked.reshape(
        group_count, row_count // dilation, dilation, head_count, row_width // head_count
    )
    choose = jnp.arange(dilation, dtype=jnp.int32)[:, None] == offsets[None, :]
    chosen = jnp.sum(
        jnp.where(choose[None, None, :, :, None], arranged, jnp.zeros((), stacked.dtype)), axis=2
    )
    return chosen.reshape(group_count, row_count // dilation, row_width)


def scatter_rows(attended, log_mass, dilation, offsets):
    query_count, head_count, head_size = attended.shape
    choose = jnp.arange(dilation, dtype=jnp.int32)[:, None] == offsets[None, :]
    spread_out = jnp.where(choose[None, :, :, None], attended[:, None, :, :], 0.0).reshape(
        query_count * dilation, head_count, head_size
    )
    spread_mass = jnp.where(choose[None, :, :], log_mass[:, None, :], masked_score).reshape(
        query_count * dilation, head_count
    )
    selected = jnp.broadcast_to(choose[None, :, :], (query_count, dilation, head_count)).reshape(
        query_count * dilation, head_count
    )
    return (spread_out, spread_mass, selected)


def attend(query_rows, key_rows, value_rows, positions, valid_limit, head_count):
    head_size = query_rows.shape[1] // head_count
    query_heads = query_rows.reshape(query_rows.shape[0], head_count, head_size)
    key_heads = key_rows.reshape(key_rows.shape[0], head_count, head_size)
    value_heads = value_rows.reshape(value_rows.shape[0], head_count, head_size)
    scores = jnp.einsum(
        "qhe,khe->hqk", query_heads, key_heads, preferred_element_type=jnp.float32
    ) / math.sqrt(head_size)
    scores = jnp.where((positions < valid_limit)[:, None, :], scores, masked_score)
    highest = jnp.max(scores, axis=-1, keepdims=True)
    exponent = jnp.exp(scores - highest)
    mass_sum = jnp.sum(exponent, axis=-1, keepdims=True)
    weights = (exponent / mass_sum).astype(jnp.bfloat16)
    attended = jnp.einsum("hqk,khe->qhe", weights, value_heads, preferred_element_type=jnp.float32)
    return (attended, (highest[..., 0] + jnp.log(mass_sum[..., 0])).T)


def body(
    tile_tokens,
    tile_gain,
    w_gate_up,
    w_down,
    layer_scale,
    fc_gain,
    w_embed,
    embed_bias,
    pre_emb,
    tile_order,
    valid_count,
    slide_gain,
    w_qkv,
    sub_gain,
    w_out,
):
    new_count, patch_count, tile_width = tile_tokens.shape
    token_rows = tile_tokens.reshape(new_count * patch_count, tile_width)
    normed = normalize(token_rows.astype(jnp.float32), tile_gain).astype(jnp.bfloat16)
    hidden_width = w_gate_up.shape[2]
    gate_up = jnp.einsum(
        "rk,gkf->grf",
        normed,
        lax.all_gather(w_gate_up, "seq", axis=1, tiled=True),
        preferred_element_type=jnp.float32,
    )
    hidden = (jax.nn.silu(gate_up[0]) * gate_up[1]).astype(jnp.bfloat16)
    pooled_hidden = jnp.mean(
        hidden.reshape(new_count, patch_count, hidden_width), axis=1, dtype=jnp.float32
    )
    everyone = lax.all_gather(pooled_hidden, "seq", axis=0, tiled=True)
    local_part = jnp.dot(everyone, w_down.astype(jnp.float32), precision=lax.Precision.HIGHEST)
    pooled_part = lax.all_to_all(local_part, "seq", split_axis=0, concat_axis=1, tiled=True)
    summed = lax.psum(pooled_part, "head")
    pooled = jnp.mean(tile_tokens, axis=1, dtype=jnp.float32) + layer_scale * summed
    feature = normalize(pooled, fc_gain).astype(jnp.bfloat16)
    new_rows = (jnp.dot(feature, w_embed, preferred_element_type=jnp.float32) + embed_bias).astype(
        jnp.bfloat16
    )
    stored = jnp.concatenate([new_rows, pre_emb], axis=0)
    block_rows = stored.shape[0]
    total_rows = tile_order.shape[0]
    peer_rows = block_rows // lax.axis_size("seq")
    device = lax.axis_index("seq")
    local_index = jnp.arange(block_rows, dtype=jnp.int32)
    inverse = (
        jnp.zeros((total_rows,), jnp.int32)
        .at[tile_order]
        .set(jnp.arange(total_rows, dtype=jnp.int32))
    )
    placed = lax.dynamic_slice_in_dim(inverse, device * block_rows, block_rows)
    target = placed // block_rows
    before = (target[:, None] == target[None, :]) & (placed[None, :] < placed[:, None])
    slot_index = target * peer_rows + jnp.sum(before, axis=1, dtype=jnp.int32)
    routing = (slot_index[None, :] == local_index[:, None]).astype(jnp.bfloat16)
    outgoing = jnp.dot(routing, stored, preferred_element_type=jnp.float32).astype(jnp.bfloat16)
    incoming = lax.all_to_all(outgoing, "seq", split_axis=0, concat_axis=0, tiled=True)
    wanted = lax.dynamic_slice_in_dim(tile_order, device * block_rows, block_rows)
    source = wanted // block_rows
    earlier = (source[:, None] == source[None, :]) & (local_index[None, :] < local_index[:, None])
    arrival = source * peer_rows + jnp.sum(earlier, axis=1, dtype=jnp.int32)
    own_part = jnp.take(incoming, arrival, axis=0)
    sequence = lax.all_gather(own_part, "head", axis=1, tiled=True)
    slide_normed = normalize(sequence.astype(jnp.float32), slide_gain).astype(jnp.bfloat16)
    projected_rows = jnp.einsum(
        "rd,gdc->grc", slide_normed, w_qkv, preferred_element_type=jnp.float32
    ).astype(jnp.bfloat16)
    cols_here = projected_rows.shape[2]
    head_count = cols_here // HEAD_DIM
    head_indices = lax.axis_index("head") * head_count + jnp.arange(head_count, dtype=jnp.int32)
    valid_limit = valid_count[0]
    row_index = device * block_rows + local_index
    near_devices = min(SPAN0, total_rows) // block_rows
    near_rows = projected_rows[1:]
    for bit_index in range(near_devices.bit_length() - 1):
        partner = from_partner(near_rows, "seq", bit_index)
        upper_half = device // (1 << bit_index) % 2 == 1
        near_rows = jnp.where(
            upper_half,
            jnp.concatenate([partner, near_rows], 1),
            jnp.concatenate([near_rows, partner], 1),
        )
    near_start = device // near_devices * near_devices * block_rows
    near_pos = jnp.broadcast_to(
        near_start + jnp.arange(near_rows.shape[1], dtype=jnp.int32),
        (head_count, near_rows.shape[1]),
    )
    near_out, near_mass = attend(
        projected_rows[0], near_rows[0], near_rows[1], near_pos, valid_limit, head_count
    )
    near_sel = jnp.ones((block_rows, head_count), dtype=bool)
    middle_level_offsets = head_indices % DILATION_SECOND
    middle_level = select_rows(projected_rows, DILATION_SECOND, middle_level_offsets)
    middle_devices = min(SPAN1, total_rows) // block_rows
    middle_key_value = middle_level[1:]
    every_row = lax.all_gather(middle_key_value, "seq", axis=1, tiled=True)
    group_rows = middle_devices * middle_key_value.shape[1]
    middle_key_value = lax.dynamic_slice_in_dim(
        every_row, device // middle_devices * group_rows, group_rows, 1
    )
    middle_start = device // middle_devices * middle_devices * block_rows
    middle_pos = (
        middle_start
        + middle_level_offsets[:, None]
        + DILATION_SECOND * jnp.arange(middle_key_value.shape[1], dtype=jnp.int32)[None, :]
    )
    middle_attention, middle_log_sum = attend(
        middle_level[0],
        middle_key_value[0],
        middle_key_value[1],
        middle_pos,
        valid_limit,
        head_count,
    )
    middle_output, middle_level_mass, middle_selected = scatter_rows(
        middle_attention, middle_log_sum, DILATION_SECOND, middle_level_offsets
    )
    distant_offsets = head_indices % DILATION_THIRD
    distant_local_rows = select_rows(projected_rows, DILATION_THIRD, distant_offsets)
    distant_key_value = lax.all_gather(distant_local_rows[1:], "seq", axis=1, tiled=True)
    distant_positions = (
        distant_offsets[:, None]
        + DILATION_THIRD * jnp.arange(distant_key_value.shape[1], dtype=jnp.int32)[None, :]
    )
    distant_attention, distant_log_sum = attend(
        distant_local_rows[0],
        distant_key_value[0],
        distant_key_value[1],
        distant_positions,
        valid_limit,
        head_count,
    )
    distant_output, distant_mass, distant_selected = scatter_rows(
        distant_attention, distant_log_sum, DILATION_THIRD, distant_offsets
    )
    outputs = jnp.stack([near_out, middle_output, distant_output])
    masses = jnp.stack([near_mass, middle_level_mass, distant_mass])
    selects = jnp.stack([near_sel, middle_selected, distant_selected])
    ceiling = jnp.max(masses, axis=0)
    shares = jnp.where(selects, jnp.exp(masses - ceiling), 0.0)
    combined = jnp.sum(shares[..., None] * outputs, axis=0) / jnp.sum(shares, axis=0)[..., None]
    combined = jnp.where((row_index < valid_limit)[:, None, None], combined, 0.0).reshape(
        block_rows, cols_here
    )
    row_total, row_square = lax.psum(
        (jnp.sum(combined, axis=1), jnp.sum(combined * combined, axis=1)), "head"
    )
    mean_value = row_total / DS
    mean_square = row_square / DS
    scaling = lax.rsqrt(mean_square - mean_value * mean_value + layer_eps)
    settled = ((combined - mean_value[:, None]) * scaling[:, None] * sub_gain).astype(jnp.bfloat16)
    partial_rows = jnp.dot(settled, w_out, preferred_element_type=jnp.float32)
    branch_sum = lax.psum_scatter(partial_rows, "head", scatter_dimension=1, tiled=True)
    return own_part.astype(jnp.float32) + branch_sum


def spread(value, axis):
    count = lax.axis_size(axis)
    return lax.all_to_all(
        jnp.broadcast_to(value[None], (count, *value.shape)), axis, split_axis=0, concat_axis=0
    )


def hidden_means(tile_tokens, tile_gain, w_gate_up, early):
    new_count, patch_count, tile_width = tile_tokens.shape
    token_rows = tile_tokens.reshape(new_count * patch_count, tile_width)
    normed = normalize(token_rows.astype(jnp.float32), tile_gain).astype(jnp.bfloat16)
    gathered = lax.all_gather(w_gate_up, "seq", axis=1, tiled=True)
    gathered, early = lax.optimization_barrier((gathered, early))
    gate_up = jnp.einsum("rk,gkf->grf", normed, gathered, preferred_element_type=jnp.float32)
    hidden = (jax.nn.silu(gate_up[0]) * gate_up[1]).astype(jnp.bfloat16)
    pooled_hidden = jnp.mean(
        hidden.reshape(new_count, patch_count, hidden.shape[1]), axis=1, dtype=jnp.float32
    )
    everyone = spread(pooled_hidden, "seq")
    return everyone.reshape(-1, hidden.shape[1]), early


def body_single(
    tile_tokens,
    tile_gain,
    w_gate_up,
    w_down,
    layer_scale,
    fc_gain,
    w_embed,
    embed_bias,
    pre_emb,
    tile_order,
    valid_count,
    slide_gain,
    w_qkv,
    sub_gain,
    w_out,
):
    new_count = tile_tokens.shape[0]
    seq_size = lax.axis_size("seq")
    head_size = lax.axis_size("head")
    device = lax.axis_index("seq")
    valid_limit = valid_count[0]
    stored = jnp.concatenate([jnp.zeros((new_count, pre_emb.shape[1]), pre_emb.dtype), pre_emb], 0)
    block_rows = stored.shape[0]
    total_rows = tile_order.shape[0]
    peer_rows = block_rows // seq_size
    local_index = jnp.arange(block_rows, dtype=jnp.int32)
    own_rows = device * block_rows + local_index
    hits = tile_order[None, :] == own_rows[:, None]
    placed = jnp.sum(
        jnp.where(hits, jnp.arange(total_rows, dtype=jnp.int32)[None, :], 0), axis=1, dtype=jnp.int32
    )
    target = placed // block_rows
    before = (target[:, None] == target[None, :]) & (placed[None, :] < placed[:, None])
    slot_index = target * peer_rows + jnp.sum(before, axis=1, dtype=jnp.int32)
    routing = (slot_index[None, :] == local_index[:, None]).astype(jnp.bfloat16)
    outgoing = jnp.dot(routing, stored, preferred_element_type=jnp.float32).astype(jnp.bfloat16)
    incoming = lax.all_to_all(outgoing, "seq", split_axis=0, concat_axis=0, tiled=True)
    wanted = lax.dynamic_slice_in_dim(tile_order, device * block_rows, block_rows)
    source = wanted // block_rows
    earlier = (source[:, None] == source[None, :]) & (local_index[None, :] < local_index[:, None])
    arrival = source * peer_rows + jnp.sum(earlier, axis=1, dtype=jnp.int32)
    arranging = (arrival[:, None] == local_index[None, :]).astype(jnp.bfloat16)
    own_pre = jnp.dot(arranging, incoming, preferred_element_type=jnp.float32).astype(jnp.bfloat16)
    sequence = lax.all_gather(own_pre, "head", axis=1, tiled=True)

    def project(rows):
        rows_normed = normalize(rows.astype(jnp.float32), slide_gain).astype(jnp.bfloat16)
        return jnp.einsum(
            "rd,gdc->grc", rows_normed, w_qkv, preferred_element_type=jnp.float32
        ).astype(jnp.bfloat16)

    projected_pre = project(sequence)
    key_value_pre = lax.all_gather(projected_pre[1:], "seq", axis=1, tiled=True)
    out_columns = lax.all_to_all(w_out, "head", split_axis=1, concat_axis=0, tiled=True)
    all_gain = lax.all_gather(sub_gain, "head", axis=0, tiled=True)
    token_means = lax.all_gather(
        jnp.mean(tile_tokens, axis=1, dtype=jnp.float32), "seq", axis=0, tiled=True
    )
    tile_count = token_means.shape[0]
    in_block = tile_order % block_rows
    tile_of = jnp.where(
        in_block < new_count, tile_order // block_rows * new_count + in_block, tile_count
    )
    holds = (tile_of[:, None] == jnp.arange(tile_count, dtype=jnp.int32)[None, :]).astype(
        jnp.bfloat16
    )
    holds_own = lax.dynamic_slice_in_dim(holds, device * block_rows, block_rows)

    early = (own_pre, projected_pre, key_value_pre, out_columns, all_gain, token_means)
    everyone, early = hidden_means(tile_tokens, tile_gain, w_gate_up, early)
    own_pre, projected_pre, key_value_pre, out_columns, all_gain, token_means = early
    local_part = jnp.dot(everyone, w_down.astype(jnp.float32), precision=lax.Precision.HIGHEST)
    parts = lax.all_gather(local_part, ("seq", "head"))
    summed = jnp.sum(parts.reshape(seq_size, head_size, tile_count, -1), axis=1)
    summed = summed.transpose(1, 0, 2).reshape(tile_count, -1)
    pooled = token_means + layer_scale * summed
    feature = normalize(pooled, fc_gain).astype(jnp.bfloat16)
    new_rows = (jnp.dot(feature, w_embed, preferred_element_type=jnp.float32) + embed_bias).astype(
        jnp.bfloat16
    )
    new_full = lax.all_gather(new_rows, "head", axis=1, tiled=True)
    projected_new = project(new_full)

    def place(held, rows):
        return jnp.dot(held, rows, preferred_element_type=jnp.float32).astype(jnp.bfloat16)

    own_part = own_pre + place(holds_own, new_rows)
    query = projected_pre[0] + place(holds_own, projected_new[0])
    key = key_value_pre[0] + place(holds, projected_new[1])
    value = key_value_pre[1] + place(holds, projected_new[2])
    cols_here = query.shape[1]
    head_count = cols_here // HEAD_DIM
    row_index = own_rows
    key_index = jnp.arange(total_rows, dtype=jnp.int32)
    key_valid = key_index < valid_limit
    attended = []
    for head in range(head_count):
        columns = slice(head * HEAD_DIM, (head + 1) * HEAD_DIM)
        head_index = lax.axis_index("head") * head_count + head
        scores = lax.dot_general(
            query[:, columns],
            key[:, columns],
            (((1,), (1,)), ((), ())),
            preferred_element_type=jnp.float32,
        ) / math.sqrt(HEAD_DIM)
        scores = jnp.where(key_valid[None, :], scores, masked_score)
        highest = jnp.max(scores, axis=1, keepdims=True)
        uses = jnp.ones((), jnp.float32)
        for dilation in (DILATION_SECOND, DILATION_THIRD):
            offset = head_index % dilation
            row_uses = (row_index % dilation == offset).astype(jnp.float32)
            key_uses = (key_index % dilation == offset).astype(jnp.float32)
            uses = uses + row_uses[:, None] * key_uses[None, :]
        weights = jnp.exp(scores - highest) * uses
        mass = jnp.sum(weights, axis=1, keepdims=True)
        summed_values = jnp.dot(
            weights.astype(jnp.bfloat16), value[:, columns], preferred_element_type=jnp.float32
        )
        attended.append(summed_values / mass)
    combined = jnp.concatenate(attended, axis=1)
    combined = jnp.where((row_index < valid_limit)[:, None], combined, 0.0)
    rows_full = lax.all_gather(combined.astype(jnp.bfloat16), "head", axis=1, tiled=True)
    rows_full = rows_full.astype(jnp.float32)
    mean_value = jnp.mean(rows_full, axis=1, keepdims=True)
    mean_square = jnp.mean(rows_full * rows_full, axis=1, keepdims=True)
    scaling = lax.rsqrt(mean_square - mean_value * mean_value + layer_eps)
    settled = ((rows_full - mean_value) * scaling * all_gain).astype(jnp.bfloat16)
    return own_part.astype(jnp.float32) + jnp.dot(
        settled, out_columns, preferred_element_type=jnp.float32
    )


def solution(mesh):
    placed = (
        P(("groups", "seq"), None, None),
        P(),
        P(None, "seq", "head"),
        P("head", "seq"),
        P(),
        P(),
        P(None, "head"),
        P("head"),
        P(("groups", "seq"), "head"),
        P("groups"),
        P("groups"),
        P(),
        P(None, None, "head"),
        P("head"),
        P("head", None),
    )


    def route(*arrays):
        single = arrays[9].shape[0] <= min(SPAN0, SPAN1)
        return (body_single if single else body)(*arrays)

    return jax.shard_map(
        route, mesh=mesh, in_specs=placed, out_specs=P(("groups", "seq"), "head"), check_vma=False
    )
```

```python
import math

import jax
import jax.numpy as jnp
from jax import lax
from jax.sharding import PartitionSpec as P

DS = 768
HEAD_DIM = 48
SPAN0 = 1024
SPAN1 = 4096
DILATION_SECOND = 4
DILATION_THIRD = 16


layer_eps = 1e-05
masked_score = -1e30


def from_partner(value, axis, bit):
    mask = 2**bit
    pairs = [(source, source ^ mask) for source in range(lax.axis_size(axis))]
    return lax.ppermute(value, axis, pairs)


def normalize(values, gain):
    centered = values - jnp.mean(values, axis=-1, keepdims=True)
    variance = jnp.mean(centered * centered, axis=-1, keepdims=True)
    return centered * lax.rsqrt(variance + layer_eps) * gain


def select_rows(stacked, dilation, offsets):
    group_count, row_count, row_width = stacked.shape
    head_count = offsets.shape[0]
    arranged = stacked.reshape(
        group_count, row_count // dilation, dilation, head_count, row_width // head_count
    )
    choose = jnp.arange(dilation, dtype=jnp.int32)[:, None] == offsets[None, :]
    chosen = jnp.sum(
        jnp.where(choose[None, None, :, :, None], arranged, jnp.zeros((), stacked.dtype)), axis=2
    )
    return chosen.reshape(group_count, row_count // dilation, row_width)


def scatter_rows(attended, log_mass, dilation, offsets):
    query_count, head_count, head_size = attended.shape
    choose = jnp.arange(dilation, dtype=jnp.int32)[:, None] == offsets[None, :]
    spread_out = jnp.where(choose[None, :, :, None], attended[:, None, :, :], 0.0).reshape(
        query_count * dilation, head_count, head_size
    )
    spread_mass = jnp.where(choose[None, :, :], log_mass[:, None, :], masked_score).reshape(
        query_count * dilation, head_count
    )
    selected = jnp.broadcast_to(choose[None, :, :], (query_count, dilation, head_count)).reshape(
        query_count * dilation, head_count
    )
    return (spread_out, spread_mass, selected)


def attend(query_rows, key_rows, value_rows, positions, valid_limit, head_count):
    head_size = query_rows.shape[1] // head_count
    query_heads = query_rows.reshape(query_rows.shape[0], head_count, head_size)
    key_heads = key_rows.reshape(key_rows.shape[0], head_count, head_size)
    value_heads = value_rows.reshape(value_rows.shape[0], head_count, head_size)
    scores = jnp.einsum(
        "qhe,khe->hqk", query_heads, key_heads, preferred_element_type=jnp.float32
    ) / math.sqrt(head_size)
    scores = jnp.where((positions < valid_limit)[:, None, :], scores, masked_score)
    highest = jnp.max(scores, axis=-1, keepdims=True)
    exponent = jnp.exp(scores - highest)
    mass_sum = jnp.sum(exponent, axis=-1, keepdims=True)
    weights = (exponent / mass_sum).astype(jnp.bfloat16)
    attended = jnp.einsum("hqk,khe->qhe", weights, value_heads, preferred_element_type=jnp.float32)
    return (attended, (highest[..., 0] + jnp.log(mass_sum[..., 0])).T)


def body(
    tile_tokens,
    tile_gain,
    w_gate_up,
    w_down,
    layer_scale,
    fc_gain,
    w_embed,
    embed_bias,
    pre_emb,
    tile_order,
    valid_count,
    slide_gain,
    w_qkv,
    sub_gain,
    w_out,
):
    new_count, patch_count, tile_width = tile_tokens.shape
    token_rows = tile_tokens.reshape(new_count * patch_count, tile_width)
    normed = normalize(token_rows.astype(jnp.float32), tile_gain).astype(jnp.bfloat16)
    hidden_width = w_gate_up.shape[2]
    gate_up = jnp.einsum(
        "rk,gkf->grf",
        normed,
        lax.all_gather(w_gate_up, "seq", axis=1, tiled=True),
        preferred_element_type=jnp.float32,
    )
    hidden = (jax.nn.silu(gate_up[0]) * gate_up[1]).astype(jnp.bfloat16)
    pooled_hidden = jnp.mean(
        hidden.reshape(new_count, patch_count, hidden_width), axis=1, dtype=jnp.float32
    )
    everyone = lax.all_gather(pooled_hidden, "seq", axis=0, tiled=True)
    local_part = jnp.dot(everyone, w_down.astype(jnp.float32), precision=lax.Precision.HIGHEST)
    pooled_part = lax.all_to_all(local_part, "seq", split_axis=0, concat_axis=1, tiled=True)
    summed = lax.psum(pooled_part, "head")
    pooled = jnp.mean(tile_tokens, axis=1, dtype=jnp.float32) + layer_scale * summed
    feature = normalize(pooled, fc_gain).astype(jnp.bfloat16)
    new_rows = (jnp.dot(feature, w_embed, preferred_element_type=jnp.float32) + embed_bias).astype(
        jnp.bfloat16
    )
    stored = jnp.concatenate([new_rows, pre_emb], axis=0)
    block_rows = stored.shape[0]
    total_rows = tile_order.shape[0]
    peer_rows = block_rows // lax.axis_size("seq")
    device = lax.axis_index("seq")
    local_index = jnp.arange(block_rows, dtype=jnp.int32)
    inverse = (
        jnp.zeros((total_rows,), jnp.int32)
        .at[tile_order]
        .set(jnp.arange(total_rows, dtype=jnp.int32))
    )
    placed = lax.dynamic_slice_in_dim(inverse, device * block_rows, block_rows)
    target = placed // block_rows
    before = (target[:, None] == target[None, :]) & (placed[None, :] < placed[:, None])
    slot_index = target * peer_rows + jnp.sum(before, axis=1, dtype=jnp.int32)
    routing = (slot_index[None, :] == local_index[:, None]).astype(jnp.bfloat16)
    outgoing = jnp.dot(routing, stored, preferred_element_type=jnp.float32).astype(jnp.bfloat16)
    incoming = lax.all_to_all(outgoing, "seq", split_axis=0, concat_axis=0, tiled=True)
    wanted = lax.dynamic_slice_in_dim(tile_order, device * block_rows, block_rows)
    source = wanted // block_rows
    earlier = (source[:, None] == source[None, :]) & (local_index[None, :] < local_index[:, None])
    arrival = source * peer_rows + jnp.sum(earlier, axis=1, dtype=jnp.int32)
    own_part = jnp.take(incoming, arrival, axis=0)
    sequence = lax.all_gather(own_part, "head", axis=1, tiled=True)
    slide_normed = normalize(sequence.astype(jnp.float32), slide_gain).astype(jnp.bfloat16)
    projected_rows = jnp.einsum(
        "rd,gdc->grc", slide_normed, w_qkv, preferred_element_type=jnp.float32
    ).astype(jnp.bfloat16)
    cols_here = projected_rows.shape[2]
    head_count = cols_here // HEAD_DIM
    head_indices = lax.axis_index("head") * head_count + jnp.arange(head_count, dtype=jnp.int32)
    valid_limit = valid_count[0]
    row_index = device * block_rows + local_index
    near_devices = min(SPAN0, total_rows) // block_rows
    near_rows = projected_rows[1:]
    for bit_index in range(near_devices.bit_length() - 1):
        partner = from_partner(near_rows, "seq", bit_index)
        upper_half = device // (1 << bit_index) % 2 == 1
        near_rows = jnp.where(
            upper_half,
            jnp.concatenate([partner, near_rows], 1),
            jnp.concatenate([near_rows, partner], 1),
        )
    near_start = device // near_devices * near_devices * block_rows
    near_pos = jnp.broadcast_to(
        near_start + jnp.arange(near_rows.shape[1], dtype=jnp.int32),
        (head_count, near_rows.shape[1]),
    )
    near_out, near_mass = attend(
        projected_rows[0], near_rows[0], near_rows[1], near_pos, valid_limit, head_count
    )
    near_sel = jnp.ones((block_rows, head_count), dtype=bool)
    middle_level_offsets = head_indices % DILATION_SECOND
    middle_level = select_rows(projected_rows, DILATION_SECOND, middle_level_offsets)
    middle_devices = min(SPAN1, total_rows) // block_rows
    middle_key_value = middle_level[1:]
    every_row = lax.all_gather(middle_key_value, "seq", axis=1, tiled=True)
    group_rows = middle_devices * middle_key_value.shape[1]
    middle_key_value = lax.dynamic_slice_in_dim(
        every_row, device // middle_devices * group_rows, group_rows, 1
    )
    middle_start = device // middle_devices * middle_devices * block_rows
    middle_pos = (
        middle_start
        + middle_level_offsets[:, None]
        + DILATION_SECOND * jnp.arange(middle_key_value.shape[1], dtype=jnp.int32)[None, :]
    )
    middle_attention, middle_log_sum = attend(
        middle_level[0],
        middle_key_value[0],
        middle_key_value[1],
        middle_pos,
        valid_limit,
        head_count,
    )
    middle_output, middle_level_mass, middle_selected = scatter_rows(
        middle_attention, middle_log_sum, DILATION_SECOND, middle_level_offsets
    )
    distant_offsets = head_indices % DILATION_THIRD
    distant_local_rows = select_rows(projected_rows, DILATION_THIRD, distant_offsets)
    distant_key_value = lax.all_gather(distant_local_rows[1:], "seq", axis=1, tiled=True)
    distant_positions = (
        distant_offsets[:, None]
        + DILATION_THIRD * jnp.arange(distant_key_value.shape[1], dtype=jnp.int32)[None, :]
    )
    distant_attention, distant_log_sum = attend(
        distant_local_rows[0],
        distant_key_value[0],
        distant_key_value[1],
        distant_positions,
        valid_limit,
        head_count,
    )
    distant_output, distant_mass, distant_selected = scatter_rows(
        distant_attention, distant_log_sum, DILATION_THIRD, distant_offsets
    )
    outputs = jnp.stack([near_out, middle_output, distant_output])
    masses = jnp.stack([near_mass, middle_level_mass, distant_mass])
    selects = jnp.stack([near_sel, middle_selected, distant_selected])
    ceiling = jnp.max(masses, axis=0)
    shares = jnp.where(selects, jnp.exp(masses - ceiling), 0.0)
    combined = jnp.sum(shares[..., None] * outputs, axis=0) / jnp.sum(shares, axis=0)[..., None]
    combined = jnp.where((row_index < valid_limit)[:, None, None], combined, 0.0).reshape(
        block_rows, cols_here
    )
    row_total, row_square = lax.psum(
        (jnp.sum(combined, axis=1), jnp.sum(combined * combined, axis=1)), "head"
    )
    mean_value = row_total / DS
    mean_square = row_square / DS
    scaling = lax.rsqrt(mean_square - mean_value * mean_value + layer_eps)
    settled = ((combined - mean_value[:, None]) * scaling[:, None] * sub_gain).astype(jnp.bfloat16)
    partial_rows = jnp.dot(settled, w_out, preferred_element_type=jnp.float32)
    branch_sum = lax.psum_scatter(partial_rows, "head", scatter_dimension=1, tiled=True)
    return own_part.astype(jnp.float32) + branch_sum


def spread(value, axis):
    count = lax.axis_size(axis)
    pieces = [value]
    for step in range(1, count):
        pairs = [(source, (source - step) % count) for source in range(count)]
        pieces.append(lax.ppermute(value, axis, pairs))
    twice = jnp.stack(pieces + pieces[:-1])
    start = (count - lax.axis_index(axis)) % count
    return lax.dynamic_slice_in_dim(twice, start, count)


def hidden_means(tile_tokens, tile_gain, w_gate_up, early):
    new_count, patch_count, tile_width = tile_tokens.shape
    token_rows = tile_tokens.reshape(new_count * patch_count, tile_width)
    share = token_rows.shape[0] // lax.axis_size("head")
    token_rows = lax.dynamic_slice_in_dim(token_rows, lax.axis_index("head") * share, share)
    normed = normalize(token_rows.astype(jnp.float32), tile_gain).astype(jnp.bfloat16)
    normed = lax.all_gather(normed, ("seq", "head"), axis=0, tiled=True)
    gates, depth, width = w_gate_up.shape
    count = lax.axis_size("seq")
    blocks = w_gate_up.reshape(gates, depth, count, width // count).transpose(2, 0, 1, 3)
    blocks = lax.all_to_all(blocks, "seq", split_axis=0, concat_axis=0)
    columns = blocks.transpose(1, 0, 2, 3).reshape(gates, count * depth, width // count)
    normed, columns, early = lax.optimization_barrier((normed, columns, early))
    gate_up = jnp.einsum("rk,gkf->grf", normed, columns, preferred_element_type=jnp.float32)
    hidden = (jax.nn.silu(gate_up[0]) * gate_up[1]).astype(jnp.bfloat16)
    pooled_hidden = jnp.mean(
        hidden.reshape(-1, patch_count, hidden.shape[1]), axis=1, dtype=jnp.float32
    )
    everyone = spread(pooled_hidden, "seq")
    return everyone.transpose(1, 0, 2).reshape(pooled_hidden.shape[0], -1), early


def body_single(
    tile_tokens,
    tile_gain,
    w_gate_up,
    w_down,
    layer_scale,
    fc_gain,
    w_embed,
    embed_bias,
    pre_emb,
    tile_order,
    valid_count,
    slide_gain,
    w_qkv,
    sub_gain,
    w_out,
):
    new_count = tile_tokens.shape[0]
    seq_size = lax.axis_size("seq")
    device = lax.axis_index("seq")
    valid_limit = valid_count[0]
    stored = jnp.concatenate([jnp.zeros((new_count, pre_emb.shape[1]), pre_emb.dtype), pre_emb], 0)
    block_rows = stored.shape[0]
    total_rows = tile_order.shape[0]
    peer_rows = block_rows // seq_size
    local_index = jnp.arange(block_rows, dtype=jnp.int32)
    own_rows = device * block_rows + local_index
    hits = tile_order[None, :] == own_rows[:, None]
    placed = jnp.sum(
        jnp.where(hits, jnp.arange(total_rows, dtype=jnp.int32)[None, :], 0), axis=1, dtype=jnp.int32
    )
    target = placed // block_rows
    before = (target[:, None] == target[None, :]) & (placed[None, :] < placed[:, None])
    slot_index = target * peer_rows + jnp.sum(before, axis=1, dtype=jnp.int32)
    routing = (slot_index[None, :] == local_index[:, None]).astype(jnp.bfloat16)
    outgoing = jnp.dot(routing, stored, preferred_element_type=jnp.float32).astype(jnp.bfloat16)
    incoming = lax.all_to_all(outgoing, "seq", split_axis=0, concat_axis=0, tiled=True)
    wanted = lax.dynamic_slice_in_dim(tile_order, device * block_rows, block_rows)
    source = wanted // block_rows
    earlier = (source[:, None] == source[None, :]) & (local_index[None, :] < local_index[:, None])
    arrival = source * peer_rows + jnp.sum(earlier, axis=1, dtype=jnp.int32)
    arranging = (arrival[:, None] == local_index[None, :]).astype(jnp.bfloat16)
    own_pre = jnp.dot(arranging, incoming, preferred_element_type=jnp.float32).astype(jnp.bfloat16)
    sequence = lax.all_gather(own_pre, "head", axis=1, tiled=True)

    def project(rows):
        rows_normed = normalize(rows.astype(jnp.float32), slide_gain).astype(jnp.bfloat16)
        return jnp.einsum(
            "rd,gdc->grc", rows_normed, w_qkv, preferred_element_type=jnp.float32
        ).astype(jnp.bfloat16)

    projected_pre = project(sequence)
    key_value_pre = (
        spread(projected_pre[1:], "seq").transpose(1, 0, 2, 3).reshape(2, total_rows, -1)
    )
    out_columns = lax.all_to_all(w_out, "head", split_axis=1, concat_axis=0, tiled=True)
    all_gain = lax.all_gather(sub_gain, "head", axis=0, tiled=True)
    token_means = spread(jnp.mean(tile_tokens, axis=1, dtype=jnp.float32), "seq")
    token_means = token_means.reshape(-1, token_means.shape[2])
    tile_count = token_means.shape[0]
    in_block = tile_order % block_rows
    tile_of = jnp.where(
        in_block < new_count, tile_order // block_rows * new_count + in_block, tile_count
    )
    holds = (tile_of[:, None] == jnp.arange(tile_count, dtype=jnp.int32)[None, :]).astype(
        jnp.bfloat16
    )
    holds_own = lax.dynamic_slice_in_dim(holds, device * block_rows, block_rows)

    early = (own_pre, projected_pre, key_value_pre, out_columns, all_gain, token_means)
    everyone, early = hidden_means(tile_tokens, tile_gain, w_gate_up, early)
    own_pre, projected_pre, key_value_pre, out_columns, all_gain, token_means = early
    local_part = jnp.dot(everyone, w_down.astype(jnp.float32), precision=lax.Precision.HIGHEST)
    summed = spread(jnp.sum(spread(local_part, "head"), axis=0), "seq")
    summed = summed.transpose(1, 0, 2).reshape(tile_count, -1)
    pooled = token_means + layer_scale * summed
    feature = normalize(pooled, fc_gain).astype(jnp.bfloat16)
    new_rows = (jnp.dot(feature, w_embed, preferred_element_type=jnp.float32) + embed_bias).astype(
        jnp.bfloat16
    )
    new_full = spread(new_rows, "head").transpose(1, 0, 2).reshape(tile_count, -1)
    projected_new = project(new_full)

    def place(held, rows):
        return jnp.dot(held, rows, preferred_element_type=jnp.float32).astype(jnp.bfloat16)

    own_part = own_pre + place(holds_own, new_rows)
    query = projected_pre[0] + place(holds_own, projected_new[0])
    key = key_value_pre[0] + place(holds, projected_new[1])
    value = key_value_pre[1] + place(holds, projected_new[2])
    cols_here = query.shape[1]
    head_count = cols_here // HEAD_DIM
    row_index = own_rows
    key_index = jnp.arange(total_rows, dtype=jnp.int32)
    key_valid = key_index < valid_limit
    attended = []
    for head in range(head_count):
        columns = slice(head * HEAD_DIM, (head + 1) * HEAD_DIM)
        head_index = lax.axis_index("head") * head_count + head
        scores = lax.dot_general(
            query[:, columns],
            key[:, columns],
            (((1,), (1,)), ((), ())),
            preferred_element_type=jnp.float32,
        ) / math.sqrt(HEAD_DIM)
        scores = jnp.where(key_valid[None, :], scores, masked_score)
        highest = jnp.max(scores, axis=1, keepdims=True)
        uses = jnp.ones((), jnp.float32)
        for dilation in (DILATION_SECOND, DILATION_THIRD):
            offset = head_index % dilation
            row_uses = (row_index % dilation == offset).astype(jnp.float32)
            key_uses = (key_index % dilation == offset).astype(jnp.float32)
            uses = uses + row_uses[:, None] * key_uses[None, :]
        weights = jnp.exp(scores - highest) * uses
        mass = jnp.sum(weights, axis=1, keepdims=True)
        summed_values = jnp.dot(
            weights.astype(jnp.bfloat16), value[:, columns], preferred_element_type=jnp.float32
        )
        attended.append(summed_values / mass)
    combined = jnp.concatenate(attended, axis=1)
    combined = jnp.where((row_index < valid_limit)[:, None], combined, 0.0)
    rows_full = lax.all_gather(combined.astype(jnp.bfloat16), "head", axis=1, tiled=True)
    rows_full = rows_full.astype(jnp.float32)
    mean_value = jnp.mean(rows_full, axis=1, keepdims=True)
    mean_square = jnp.mean(rows_full * rows_full, axis=1, keepdims=True)
    scaling = lax.rsqrt(mean_square - mean_value * mean_value + layer_eps)
    settled = ((rows_full - mean_value) * scaling * all_gain).astype(jnp.bfloat16)
    return own_part.astype(jnp.float32) + jnp.dot(
        settled, out_columns, preferred_element_type=jnp.float32
    )


def solution(mesh):
    placed = (
        P(("groups", "seq"), None, None),
        P(),
        P(None, "seq", "head"),
        P("head", "seq"),
        P(),
        P(),
        P(None, "head"),
        P("head"),
        P(("groups", "seq"), "head"),
        P("groups"),
        P("groups"),
        P(),
        P(None, None, "head"),
        P("head"),
        P("head", None),
    )


    def route(*arrays):
        single = arrays[9].shape[0] <= min(SPAN0, SPAN1)
        return (body_single if single else body)(*arrays)

    return jax.shard_map(
        route, mesh=mesh, in_specs=placed, out_specs=P(("groups", "seq"), "head"), check_vma=False
    )
```
